32 devices in a mesh: dp: 1 (over z), y: 4 (over y), x: 8 (over x, core).
Axes of the slice: x: 4, y: 4, z: 1, core: 2. Of those that a mesh axis runs over, the one named last changes fastest.
The devices are a block of a 4x4x8 slice.
Arguments:
- tokens: int32 [3, 256], P(None, 'dp')
- lengths: int32 [256], P('dp')
- choices: int32 [3, 256, 8], P(None, 'dp')
- emb_table: bfloat16 [50304, 2048], P(None, 'x')
- k_cache: bfloat16 [256, 128, 16, 128], P('dp', None, 'y')
- v_cache: bfloat16 [256, 128, 16, 128], P('dp', None, 'y')
- g_attn: bfloat16 [2048], P('x')
- w_q: bfloat16 [2048, 2048], P('x', 'y')
- w_k: bfloat16 [2048, 2048], P('x', 'y')
- w_v: bfloat16 [2048, 2048], P('x', 'y')
- w_o: bfloat16 [2048, 2048], P('y', 'x')
- g_ffn: bfloat16 [2048], P('x')
- w_router: bfloat16 [2048, 64], P('x')
- w_act: bfloat16 [64, 2048, 1024], P(None, 'x', 'y')
- w_lin: bfloat16 [64, 2048, 1024], P(None, 'x', 'y')
- w_down: bfloat16 [64, 1024, 2048], P(None, 'y', 'x')
Outputs:
- output 1: bfloat16 [3, 256, 2048], P(None, 'dp', 'x')
- output 2: bfloat16 [256, 128, 16, 128], P('dp', None, 'y')
- output 3: bfloat16 [256, 128, 16, 128], P('dp', None, 'y')
All inputs are finite; a program needn't handle non-finite values.
Results may differ from the reference program's by a relative error of at most 0.0126822.
Values are sent between devices in bfloat16 or wider.
A program may use at most 768 MiB of HBM per device.

```python
import math
import jax
import jax.numpy as jnp
from jax import lax

BATCH = 256
SEQ = 128
D = 2048
HEADS = 16
KV_HEADS = 16
HEAD = 128
FF = 1024
EXPERTS = 64
TOP = 8
VOCAB = 50304
STEPS = 3

EPS = 1e-5
ROPE_BASE = 1.0e6
LOG_SEQ = int(math.log2(SEQ))
HOT_COUNT = max(1, EXPERTS // 8)
GROUP_SIZE = HEADS // KV_HEADS


def draw_lengths(key_a, key_b, key_c):
    exponent = jax.random.randint(key_a, (BATCH,), 0, LOG_SEQ + 1)
    len_limit = jnp.minimum(jnp.left_shift(jnp.ones((BATCH,), jnp.int32), exponent), SEQ - 3)
    raw_draw = jax.random.randint(key_b, (BATCH,), 0, 1 << 30)
    lengths = 1 + raw_draw % len_limit
    pick_row = jax.random.randint(key_c, (), 0, BATCH)
    row_ids = jnp.arange(BATCH)
    lengths = jnp.where(row_ids == pick_row, SEQ - 3, lengths)
    lengths = jnp.where(row_ids == (pick_row + 1) % BATCH, 1, lengths)
    return lengths.astype(jnp.int32)


def draw_choices(key_a, key_b):
    expert_rank = jax.random.permutation(key_a, EXPERTS)
    hot_bonus = jnp.where(expert_rank < HOT_COUNT, EXPERTS, 0)
    noise_int = jax.random.randint(key_b, (STEPS, BATCH, EXPERTS), 0, 2 * EXPERTS)
    scores = (noise_int + hot_bonus) * EXPERTS + jnp.arange(EXPERTS)
    return lax.top_k(scores, TOP)[1].astype(jnp.int32)


def normal_weights(key_w, shape_w, scale_w):
    return (jax.random.normal(key_w, shape_w, jnp.float32) * scale_w).astype(jnp.bfloat16)


def setup_inputs(seed: int = 0, part: int = 0) -> dict:
    base_key = jax.random.key(seed)
    weight_keys = jax.random.split(base_key, 12)
    part_keys = jax.random.split(jax.random.fold_in(base_key, part), 8)
    tokens = jax.random.randint(part_keys[0], (STEPS, BATCH), 0, VOCAB)
    lengths = draw_lengths(part_keys[1], part_keys[2], part_keys[3])
    choices = draw_choices(part_keys[4], part_keys[5])
    k_cache = normal_weights(part_keys[6], (BATCH, SEQ, KV_HEADS, HEAD), 1.0)
    v_cache = normal_weights(part_keys[7], (BATCH, SEQ, KV_HEADS, HEAD), 1.0)
    ramp_rate = jax.random.uniform(weight_keys[0], (), jnp.float32, 0.6, 1.2)
    col_scale = jnp.exp(ramp_rate * jnp.linspace(-1.0, 1.0, D))
    emb_table = (jax.random.normal(weight_keys[1], (VOCAB, D), jnp.float32) * col_scale).astype(jnp.bfloat16)
    g_attn = (1.0 + 0.3 * jax.random.normal(weight_keys[2], (D,), jnp.float32)).astype(jnp.bfloat16)
    w_q = normal_weights(weight_keys[3], (D, HEADS * HEAD), D ** -0.5)
    w_k = normal_weights(weight_keys[4], (D, KV_HEADS * HEAD), D ** -0.5)
    w_v = normal_weights(weight_keys[5], (D, KV_HEADS * HEAD), D ** -0.5)
    w_o = normal_weights(weight_keys[6], (HEADS * HEAD, D), (HEADS * HEAD) ** -0.5)
    g_ffn = (1.0 + 0.3 * jax.random.normal(weight_keys[7], (D,), jnp.float32)).astype(jnp.bfloat16)
    w_router = normal_weights(weight_keys[8], (D, EXPERTS), 1.5 * D ** -0.5)
    w_act = normal_weights(weight_keys[9], (EXPERTS, D, FF), D ** -0.5)
    w_lin = normal_weights(weight_keys[10], (EXPERTS, D, FF), D ** -0.5)
    w_down = normal_weights(weight_keys[11], (EXPERTS, FF, D), FF ** -0.5)
    return dict(tokens=tokens, lengths=lengths, choices=choices, emb_table=emb_table, k_cache=k_cache, v_cache=v_cache, g_attn=g_attn, w_q=w_q, w_k=w_k, w_v=w_v, w_o=w_o, g_ffn=g_ffn, w_router=w_router, w_act=w_act, w_lin=w_lin, w_down=w_down)


def rms_norm(x_val, gain_vec):
    x_f32 = x_val.astype(jnp.float32)
    meansq = jnp.sum(x_f32 * x_f32, axis=-1, keepdims=True) / D
    return (x_f32 * lax.rsqrt(meansq + EPS) * gain_vec.astype(jnp.float32)).astype(jnp.bfloat16)


def rotate(vectors, positions):
    half_dim = HEAD // 2
    inv_freq = ROPE_BASE ** (-(jnp.arange(half_dim).astype(jnp.float32) * 2.0 / HEAD))
    angles = positions.astype(jnp.float32)[:, None, None] * inv_freq
    cosine = jnp.cos(angles)
    sine_val = jnp.sin(angles)
    first_half = vectors[..., :half_dim].astype(jnp.float32)
    second_half = vectors[..., half_dim:].astype(jnp.float32)
    return jnp.concatenate([first_half * cosine - second_half * sine_val, second_half * cosine + first_half * sine_val], axis=-1).astype(jnp.bfloat16)


def attend_row(row_args):
    q_row, key_row, val_row, pos_row = row_args
    scores = jnp.einsum('kgh,skh->kgs', q_row.astype(jnp.float32), key_row.astype(jnp.float32)) * HEAD ** -0.5
    valid_mask = jnp.arange(SEQ) <= pos_row
    scores = jnp.where(valid_mask, scores, -1.0e30)
    peak_val = jnp.max(scores, axis=-1, keepdims=True)
    weight = jnp.where(valid_mask, jnp.exp(scores - peak_val), 0.0)
    total_w = jnp.sum(weight, axis=-1, keepdims=True)
    mixed_out = jnp.einsum('kgs,skh->kgh', weight.astype(jnp.bfloat16).astype(jnp.float32), val_row.astype(jnp.float32))
    return (mixed_out / total_w).astype(jnp.bfloat16)


def reference(tokens, lengths, choices, emb_table, k_cache, v_cache, g_attn, w_q, w_k, w_v, w_o, g_ffn, w_router, w_act, w_lin, w_down):
    slot_ids = jnp.arange(SEQ)
    expert_ids = jnp.arange(EXPERTS)

    def one_step(carry, step_in):
        key_cache, val_cache = carry
        tok_row, choice_row, step_idx = step_in
        positions = lengths + step_idx
        x_in = emb_table[tok_row]
        normed = rms_norm(x_in, g_attn)
        queries = rotate(jnp.dot(normed, w_q, preferred_element_type=jnp.float32).astype(jnp.bfloat16).reshape(BATCH, HEADS, HEAD), positions)
        new_keys = rotate(jnp.dot(normed, w_k, preferred_element_type=jnp.float32).astype(jnp.bfloat16).reshape(BATCH, KV_HEADS, HEAD), positions)
        new_vals = jnp.dot(normed, w_v, preferred_element_type=jnp.float32).astype(jnp.bfloat16).reshape(BATCH, KV_HEADS, HEAD)
        hit_mask = (slot_ids[None, :] == positions[:, None])[:, :, None, None]
        key_cache = jnp.where(hit_mask, new_keys[:, None], key_cache)
        val_cache = jnp.where(hit_mask, new_vals[:, None], val_cache)
        grouped = queries.reshape(BATCH, KV_HEADS, GROUP_SIZE, HEAD)
        mixed = lax.map(attend_row, (grouped, key_cache, val_cache, positions)).reshape(BATCH, HEADS * HEAD)
        x_mid = (x_in.astype(jnp.float32) + jnp.dot(mixed, w_o, preferred_element_type=jnp.float32)).astype(jnp.bfloat16)
        normed2 = rms_norm(x_mid, g_ffn)
        logits = jnp.dot(normed2, w_router, preferred_element_type=jnp.float32)
        gate_val = jax.nn.softmax(jnp.take_along_axis(logits, choice_row, axis=1), axis=-1)
        onehot = choice_row[:, :, None] == expert_ids[None, None, :]
        coef = jnp.sum(jnp.where(onehot, gate_val[:, :, None], 0.0), axis=1)

        def expert_out(expert_args):
            act_w, lin_w, down_w, coef_col = expert_args
            act_f32 = jnp.dot(normed2, act_w, preferred_element_type=jnp.float32)
            lin_f32 = jnp.dot(normed2, lin_w, preferred_element_type=jnp.float32)
            unit_bf16 = (coef_col[:, None] * jax.nn.silu(act_f32) * lin_f32).astype(jnp.bfloat16)
            return jnp.dot(unit_bf16, down_w, preferred_element_type=jnp.float32)

        moe_sum = jnp.sum(lax.map(expert_out, (w_act, w_lin, w_down, coef.T)), axis=0)
        hidden_out = (x_mid.astype(jnp.float32) + moe_sum).astype(jnp.bfloat16)
        return (key_cache, val_cache), hidden_out

    (k_out, v_out), hidden_out = lax.scan(one_step, (k_cache, v_cache), (tokens, choices, jnp.arange(STEPS)))
    return hidden_out, k_out, v_out
```

```python
import functools

import jax
import jax.numpy as jnp
from jax import lax
from jax.experimental import pallas as pl
from jax.experimental.pallas import tpu as pltpu
from jax.sharding import PartitionSpec as P

EPS = 1e-5
ROPE_BASE = 1.0e6
TILE = 128
BF16 = jnp.bfloat16
F32 = jnp.float32


def shard_norm(x_val, gain_vec, width_full):
    x_f32 = x_val.astype(F32)
    sq_total = lax.psum(jnp.sum(x_f32 * x_f32, axis=-1, keepdims=True), 'x')
    return (x_f32 * lax.rsqrt(sq_total / width_full + EPS) * gain_vec.astype(F32)).astype(BF16)


def rotate(vectors, positions):
    head_dim = vectors.shape[-1]
    half_dim = head_dim // 2
    inv_freq = ROPE_BASE ** (-(jnp.arange(half_dim, dtype=F32) * 2.0 / head_dim))
    angles = (positions.astype(F32)[:, None] * inv_freq[None, :])[:, None, :]
    cosine = jnp.cos(angles)
    sine_val = jnp.sin(angles)
    first_half = vectors[..., :half_dim].astype(F32)
    second_half = vectors[..., half_dim:].astype(F32)
    return jnp.concatenate([first_half * cosine - second_half * sine_val, second_half * cosine + first_half * sine_val], axis=-1).astype(BF16)


def attention(queries, key_cache, val_cache, positions):
    head_dim = queries.shape[-1]
    scores = jnp.einsum('tbkh,bskh->bkts', queries, key_cache, preferred_element_type=F32) * head_dim ** -0.5
    valid_mask = (jnp.arange(key_cache.shape[1])[None, None, :] <= positions.T[:, :, None])[:, None]
    scores = jnp.where(valid_mask, scores, -1.0e30)
    peak_val = jnp.max(scores, axis=-1, keepdims=True)
    weight = jnp.where(valid_mask, jnp.exp(scores - peak_val), 0.0)
    total_w = jnp.sum(weight, axis=-1, keepdims=True)
    mixed_out = jnp.einsum('bkts,bskh->bkth', weight.astype(BF16), val_cache, preferred_element_type=F32)
    return (mixed_out / total_w).astype(BF16).transpose(2, 0, 1, 3)


def write_slots(cache_arr, new_rows, lengths):
    slots = jnp.arange(cache_arr.shape[1])[None, :]
    for step_idx in range(new_rows.shape[0]):
        hit_mask = (slots == (lengths + step_idx)[:, None])[:, :, None, None]
        cache_arr = jnp.where(hit_mask, new_rows[step_idx][:, None], cache_arr)
    return cache_arr


def up_kernel(per_step, tile, off_ref, pos_ref, h_ref, act_ref, lin_ref, out_ref):
    step = pl.program_id(0)

    @pl.when(step == 0)
    def _():
        out_ref[...] = jnp.zeros_like(out_ref)

    tokens = h_ref.shape[0]
    width = act_ref.shape[2]
    row_iota = lax.broadcasted_iota(jnp.int32, (tile, tokens), 0)
    for j in range(per_step):
        e = step * per_step + j
        lo, hi = off_ref[e], off_ref[e + 1]
        pos_row = pos_ref[j]

        def visit(i, carry):
            base = pl.multiple_of(i * tile, tile)
            pick = (jnp.broadcast_to(pos_row - base, (tile, tokens)) == row_iota).astype(F32).astype(BF16)
            rows = jnp.dot(pick, h_ref[...], preferred_element_type=F32).astype(BF16)
            act = jnp.dot(rows, act_ref[j], preferred_element_type=F32).astype(BF16)
            lin = jnp.dot(rows, lin_ref[j], preferred_element_type=F32).astype(BF16)
            out_ref[pl.ds(base, tile), :width] += act
            out_ref[pl.ds(base, tile), width:] += lin
            return carry

        lax.fori_loop(lo // tile, (hi + tile - 1) // tile, visit, 0)


def down_kernel(per_step, tile, off_ref, pos_ref, u_ref, w_ref, out_ref, acc_ref, mix_ref):
    step = pl.program_id(0)

    @pl.when(step == 0)
    def _():
        acc_ref[...] = jnp.zeros_like(acc_ref)

    tokens = out_ref.shape[0]
    row_iota = lax.broadcasted_iota(jnp.int32, (tile, tokens), 0)
    for j in range(per_step):
        e = step * per_step + j
        lo, hi = off_ref[e], off_ref[e + 1]
        pos_row = pos_ref[j]
        mix_ref[...] = jnp.zeros_like(mix_ref)

        def visit(i, carry):
            base = pl.multiple_of(i * tile, tile)
            pick = (jnp.broadcast_to(pos_row - base, (tile, tokens)) == row_iota).astype(F32).astype(BF16)
            mix_ref[...] += lax.dot_general(pick, u_ref[pl.ds(base, tile), :], (((0,), (0,)), ((), ())), preferred_element_type=F32).astype(BF16)
            return carry

        lax.fori_loop(lo // tile, (hi + tile - 1) // tile, visit, 0)
        acc_ref[...] += jnp.dot(mix_ref[...], w_ref[j], preferred_element_type=F32)

    @pl.when(step == pl.num_programs(0) - 1)
    def _():
        out_ref[...] = acc_ref[...].astype(BF16)


def experts_up(offsets, pos_rows, normed, w_act, w_lin, pairs):
    experts, depth, width = w_act.shape
    tokens = normed.shape[0]
    per_step = 4
    return pl.pallas_call(
        functools.partial(up_kernel, per_step, TILE),
        out_shape=jax.ShapeDtypeStruct((pairs, 2 * width), BF16),
        grid_spec=pltpu.PrefetchScalarGridSpec(
            num_scalar_prefetch=1,
            grid=(experts // per_step,),
            in_specs=[
                pl.BlockSpec((per_step, 1, tokens), lambda s, off: (s, 0, 0)),
                pl.BlockSpec((tokens, depth), lambda s, off: (0, 0)),
                pl.BlockSpec((per_step, depth, width), lambda s, off: (s, 0, 0)),
                pl.BlockSpec((per_step, depth, width), lambda s, off: (s, 0, 0)),
            ],
            out_specs=pl.BlockSpec((pairs, 2 * width), lambda s, off: (0, 0)),
        ),
        compiler_params=pltpu.CompilerParams(dimension_semantics=("arbitrary",), vmem_limit_bytes=48 << 20),
        cost_estimate=pl.CostEstimate(flops=12 << 30, bytes_accessed=24 << 20, transcendentals=0),
        name="experts_up",
    )(offsets, pos_rows, normed, w_act, w_lin)


def experts_down(offsets, pos_rows, unit, w_down):
    experts, width, depth = w_down.shape
    tokens = pos_rows.shape[2]
    per_step = 4
    return pl.pallas_call(
        functools.partial(down_kernel, per_step, TILE),
        out_shape=jax.ShapeDtypeStruct((tokens, depth), BF16),
        grid_spec=pltpu.PrefetchScalarGridSpec(
            num_scalar_prefetch=1,
            grid=(experts // per_step,),
            in_specs=[
                pl.BlockSpec((per_step, 1, tokens), lambda s, off: (s, 0, 0)),
                pl.BlockSpec(unit.shape, lambda s, off: (0, 0)),
                pl.BlockSpec((per_step, width, depth), lambda s, off: (s, 0, 0)),
            ],
            out_specs=pl.BlockSpec((tokens, depth), lambda s, off: (0, 0)),
            scratch_shapes=[pltpu.VMEM((tokens, depth), F32), pltpu.VMEM((tokens, width), BF16)],
        ),
        compiler_params=pltpu.CompilerParams(dimension_semantics=("arbitrary",), vmem_limit_bytes=40 << 20),
        cost_estimate=pl.CostEstimate(flops=12 << 30, bytes_accessed=12 << 20, transcendentals=0),
        name="experts_down",
    )(offsets, pos_rows, unit, w_down)


def solution(mesh):
    nx = mesh.shape['x']
    cache_spec = P('dp', None, 'y', None)
    in_specs = (P(None, 'dp'), P('dp'), P(None, 'dp', None), P(None, 'x'), cache_spec, cache_spec, P('x'), P('x', 'y'), P('x', 'y'), P('x', 'y'), P('y', 'x'), P('x'), P('x', None), P(None, 'x', 'y'), P(None, 'x', 'y'), P(None, 'y', 'x'))
    out_specs = (P(None, 'dp', 'x'), cache_spec, cache_spec)

    def per_device(tokens, lengths, choices, emb_table, k_cache, v_cache, g_attn, w_q, w_k, w_v, w_o, g_ffn, w_router, w_act, w_lin, w_down):
        steps, batch = tokens.shape
        top = choices.shape[2]
        heads, head_dim = k_cache.shape[2], k_cache.shape[3]
        cols = heads * head_dim
        width_full = emb_table.shape[1] * nx
        experts = w_act.shape[0]
        my_x = lax.axis_index('x')
        part = batch // nx
        rows = steps * batch
        pairs = rows * top

        def to_rows(arr):
            return arr.reshape((steps, nx, part) + arr.shape[2:]).swapaxes(0, 1).reshape((rows,) + arr.shape[2:])

        def from_rows(arr):
            return arr.reshape((nx, steps, part) + arr.shape[1:]).swapaxes(0, 1).reshape((steps, batch) + arr.shape[1:])

        choice_rows = to_rows(choices)
        member = jnp.any(choice_rows[:, :, None] == jnp.arange(experts)[None, None, :], axis=1)
        member_f = member.astype(F32)
        before = (jnp.arange(rows)[None, :] < jnp.arange(rows)[:, None]).astype(BF16)
        rank = jnp.dot(before, member.astype(BF16), preferred_element_type=F32)
        counts = jnp.sum(member_f, axis=0)
        ends = jnp.cumsum(counts)
        starts = ends - counts
        pos = jnp.where(member, rank + starts[None, :], -1.0)
        pos_rows = pos.T.astype(jnp.int32)[:, None, :]
        offsets = jnp.concatenate([starts, ends[-1:]]).astype(jnp.int32)
        share = pairs // nx
        own = (my_x * share + jnp.arange(share)).astype(F32)
        own_expert = ((own[:, None] >= starts[None, :]) & (own[:, None] < ends[None, :])).astype(F32)
        own_pos = lax.dot_general(own_expert, pos, (((1,), (1,)), ((), ())), precision=lax.Precision.HIGHEST, preferred_element_type=F32)
        own_token = (own_pos == own[:, None]).astype(F32)

        x_in = jnp.take(emb_table, to_rows(tokens), axis=0)
        normed = shard_norm(x_in, g_attn, width_full)
        proj_part = jnp.concatenate([jnp.dot(normed, w, preferred_element_type=F32).astype(BF16) for w in (w_q, w_k, w_v)], axis=1)
        proj = lax.psum_scatter(proj_part, 'x', scatter_dimension=0, tiled=True)
        my_lengths = lax.dynamic_slice_in_dim(lengths, my_x * part, part)
        my_positions = my_lengths[None, :] + jnp.arange(steps)[:, None]
        flat_positions = my_positions.reshape(-1)
        queries = rotate(proj[:, :cols].reshape(-1, heads, head_dim), flat_positions)
        new_keys = rotate(proj[:, cols:2 * cols].reshape(-1, heads, head_dim), flat_positions)
        new_vals = proj[:, 2 * cols:].reshape(-1, heads, head_dim)

        def split(arr):
            return arr.reshape(steps, part, heads, head_dim)

        my_keys = write_slots(lax.dynamic_slice_in_dim(k_cache, my_x * part, part), split(new_keys), my_lengths)
        my_vals = write_slots(lax.dynamic_slice_in_dim(v_cache, my_x * part, part), split(new_vals), my_lengths)
        mixed = attention(split(queries), my_keys, my_vals, my_positions).reshape(-1, cols)
        mixed_all = lax.all_gather(mixed, 'x', axis=0, tiled=True)

        new_kv = jnp.concatenate([new_keys.reshape(-1, cols), proj[:, 2 * cols:]], axis=1)
        kv_all = from_rows(lax.all_gather(new_kv, 'x', axis=0, tiled=True))
        k_out = write_slots(k_cache, kv_all[:, :, :cols].reshape(steps, batch, heads, head_dim), lengths)
        v_out = write_slots(v_cache, kv_all[:, :, cols:].reshape(steps, batch, heads, head_dim), lengths)

        attn_sum = lax.psum(jnp.dot(mixed_all, w_o, preferred_element_type=F32).astype(BF16), 'y')
        x_mid = (x_in.astype(F32) + attn_sum.astype(F32)).astype(BF16)
        normed2 = shard_norm(x_mid, g_ffn, width_full)
        logits = lax.psum(jnp.dot(normed2, w_router, preferred_element_type=F32), 'x')
        masked = jnp.where(member, logits, -jnp.inf)
        expd = jnp.exp(masked - jnp.max(masked, axis=1, keepdims=True))
        coef = expd / jnp.sum(expd, axis=1, keepdims=True)
        own_gate = jnp.sum(own_expert * jnp.dot(own_token, coef, precision=lax.Precision.HIGHEST, preferred_element_type=F32), axis=1, keepdims=True)

        hidden_part = experts_up(offsets, pos_rows, normed2, w_act, w_lin, pairs)
        hidden = lax.psum_scatter(hidden_part, 'x', scatter_dimension=0, tiled=True)
        width = w_act.shape[2]
        unit = (own_gate * jax.nn.silu(hidden[:, :width].astype(F32)) * hidden[:, width:].astype(F32)).astype(BF16)
        unit_all = lax.all_gather(unit, 'x', axis=0, tiled=True)
        moe_sum = lax.psum(experts_down(offsets, pos_rows, unit_all, w_down), 'y')
        hidden_out = (x_mid.astype(F32) + moe_sum.astype(F32)).astype(BF16)
        return from_rows(hidden_out), k_out, v_out

    return jax.shard_map(per_device, mesh=mesh, in_specs=in_specs, out_specs=out_specs, check_vma=False)
```

```python
import functools

import jax
import jax.numpy as jnp
from jax import lax
from jax.experimental import pallas as pl
from jax.experimental.pallas import tpu as pltpu
from jax.sharding import PartitionSpec as P

EPS = 1e-5
ROPE_BASE = 1.0e6
TILE = 128
CHUNKS = 1
BF16 = jnp.bfloat16
F32 = jnp.float32
MESH = pl.DeviceIdType.MESH


def shard_norm(x_val, gain_vec, width_full, n, ident):
    x_f32 = x_val.astype(F32)
    rows = x_val.shape[0]
    sq_part = jnp.sum(x_f32 * x_f32, axis=-1).reshape(-1, 128)
    sq_total = jnp.sum(small_gather(sq_part, 'x', n, ident), axis=0).reshape(rows, 1)
    return (x_f32 * lax.rsqrt(sq_total / width_full + EPS) * gain_vec.astype(F32)).astype(BF16)


def rotate(vectors, positions):
    head_dim = vectors.shape[-1]
    half_dim = head_dim // 2
    inv_freq = ROPE_BASE ** (-(jnp.arange(half_dim, dtype=F32) * 2.0 / head_dim))
    angles = (positions.astype(F32)[:, None] * inv_freq[None, :])[:, None, :]
    cosine = jnp.cos(angles)
    sine_val = jnp.sin(angles)
    first_half = vectors[..., :half_dim].astype(F32)
    second_half = vectors[..., half_dim:].astype(F32)
    return jnp.concatenate([first_half * cosine - second_half * sine_val, second_half * cosine + first_half * sine_val], axis=-1).astype(BF16)


def attention(queries, new_keys, new_vals, key_cache, val_cache, lengths):
    head_dim = queries.shape[-1]
    steps = queries.shape[0]
    old = jnp.einsum('tbkh,bskh->bkts', queries, key_cache, preferred_element_type=F32) * head_dim ** -0.5
    new = jnp.sum(queries.astype(F32)[:, None] * new_keys.astype(F32)[None], axis=-1).transpose(2, 3, 0, 1) * head_dim ** -0.5
    old_mask = (jnp.arange(key_cache.shape[1])[None, :] < lengths[:, None])[:, None, None, :]
    new_mask = (jnp.arange(steps)[None, :] <= jnp.arange(steps)[:, None])[None, None]
    old = jnp.where(old_mask, old, -1.0e30)
    new = jnp.where(new_mask, new, -1.0e30)
    peak_val = jnp.maximum(jnp.max(old, axis=-1, keepdims=True), jnp.max(new, axis=-1, keepdims=True))
    w_old = jnp.where(old_mask, jnp.exp(old - peak_val), 0.0)
    w_new = jnp.where(new_mask, jnp.exp(new - peak_val), 0.0)
    total_w = jnp.sum(w_old, axis=-1, keepdims=True) + jnp.sum(w_new, axis=-1, keepdims=True)
    mixed = jnp.einsum('bkts,bskh->bkth', w_old.astype(BF16), val_cache, preferred_element_type=F32)
    vals = new_vals.astype(F32).transpose(1, 2, 0, 3)
    mixed = mixed + jnp.sum(w_new.astype(BF16).astype(F32)[..., None] * vals[:, :, None], axis=3)
    return (mixed / total_w).astype(BF16).transpose(2, 0, 1, 3)


def up_kernel(per_step, tile, off_ref, rows_ref, act_ref, lin_ref, out_ref):
    step = pl.program_id(0)

    @pl.when(step == 0)
    def _():
        out_ref[...] = jnp.zeros_like(out_ref)

    depth, width = act_ref.shape[1], act_ref.shape[2]
    row_iota = lax.broadcasted_iota(jnp.int32, (tile, depth), 0)
    last = rows_ref.shape[0] // tile - 1

    def products(j, i):
        lo, hi = off_ref[step * per_step + j], off_ref[step * per_step + j + 1]
        base = pl.multiple_of(i * tile, tile)
        rows = rows_ref[pl.ds(base, tile), :].astype(F32)
        rows = jnp.where((row_iota >= lo - base) & (row_iota < hi - base), rows, 0.0).astype(BF16)
        act = jnp.dot(rows, act_ref[j], preferred_element_type=F32).astype(BF16)
        lin = jnp.dot(rows, lin_ref[j], preferred_element_type=F32).astype(BF16)
        return base, act, lin

    def add(base, act, lin):
        out_ref[pl.ds(base, tile), :width] += act
        out_ref[pl.ds(base, tile), width:] += lin

    for j in range(0, per_step, 2):
        firsts = [jnp.minimum(off_ref[step * per_step + k] // tile, last) for k in (j, j + 1)]
        for item in [products(k, i) for k, i in zip((j, j + 1), firsts)]:
            add(*item)
        for k, i in zip((j, j + 1), firsts):

            def visit(i, carry):
                add(*products(k, i))
                return carry

            lax.fori_loop(i + 1, (off_ref[step * per_step + k + 1] + tile - 1) // tile, visit, 0)


def down_kernel(per_step, tile, off_ref, u_ref, w_ref, out_ref, acc_ref):
    step = pl.program_id(0)

    @pl.when(step == 0)
    def _():
        acc_ref[...] = jnp.zeros_like(acc_ref)

    width, depth = w_ref.shape[1], w_ref.shape[2]
    row_iota = lax.broadcasted_iota(jnp.int32, (tile, width), 0)
    last = u_ref.shape[0] // tile - 1

    def product(j, i):
        lo, hi = off_ref[step * per_step + j], off_ref[step * per_step + j + 1]
        base = pl.multiple_of(i * tile, tile)
        rows = u_ref[pl.ds(base, tile), :].astype(F32)
        rows = jnp.where((row_iota >= lo - base) & (row_iota < hi - base), rows, 0.0).astype(BF16)
        return base, jnp.dot(rows, w_ref[j], preferred_element_type=F32)

    def add(base, out):
        acc_ref[pl.ds(base, tile), :] += out

    for j in range(0, per_step, 2):
        firsts = [jnp.minimum(off_ref[step * per_step + k] // tile, last) for k in (j, j + 1)]
        for item in [product(k, i) for k, i in zip((j, j + 1), firsts)]:
            add(*item)
        for k, i in zip((j, j + 1), firsts):

            def visit(i, carry):
                add(*product(k, i))
                return carry

            lax.fori_loop(i + 1, (off_ref[step * per_step + k + 1] + tile - 1) // tile, visit, 0)

    @pl.when(step == pl.num_programs(0) - 1)
    def _():
        def cut(i, carry):
            at = pl.ds(pl.multiple_of(i * tile, tile), tile)
            rest = acc_ref[at, :]
            for k in range(3):
                term = rest.astype(BF16)
                out_ref[at, k * depth:(k + 1) * depth] = term
                rest = rest - term.astype(F32)
            return carry

        lax.fori_loop(0, acc_ref.shape[0] // tile, cut, 0)


def experts_up(offsets, rows, w_act, w_lin):
    experts, depth, width = w_act.shape
    pairs = rows.shape[0]
    per_step = 4
    return pl.pallas_call(
        functools.partial(up_kernel, per_step, TILE),
        out_shape=jax.ShapeDtypeStruct((pairs, 2 * width), BF16),
        grid_spec=pltpu.PrefetchScalarGridSpec(
            num_scalar_prefetch=1,
            grid=(experts // per_step,),
            in_specs=[
                pl.BlockSpec((pairs, depth), lambda s, off: (0, 0), pipeline_mode=pl.Buffered(1)),
                pl.BlockSpec((per_step, depth, width), lambda s, off: (s, 0, 0)),
                pl.BlockSpec((per_step, depth, width), lambda s, off: (s, 0, 0)),
            ],
            out_specs=pl.BlockSpec((pairs, 2 * width), lambda s, off: (0, 0), pipeline_mode=pl.Buffered(1)),
        ),
        compiler_params=pltpu.CompilerParams(dimension_semantics=("arbitrary",), vmem_limit_bytes=40 << 20),
        cost_estimate=pl.CostEstimate(flops=12 << 30, bytes_accessed=24 << 20, transcendentals=0),
        name="experts_up",
    )(offsets, rows, w_act, w_lin)


def experts_down(offsets, unit, w_down):
    experts, width, depth = w_down.shape
    pairs = unit.shape[0]
    per_step = 4
    return pl.pallas_call(
        functools.partial(down_kernel, per_step, TILE),
        out_shape=jax.ShapeDtypeStruct((pairs, 3 * depth), BF16),
        grid_spec=pltpu.PrefetchScalarGridSpec(
            num_scalar_prefetch=1,
            grid=(experts // per_step,),
            in_specs=[
                pl.BlockSpec(unit.shape, lambda s, off: (0, 0), pipeline_mode=pl.Buffered(1)),
                pl.BlockSpec((per_step, width, depth), lambda s, off: (s, 0, 0)),
            ],
            out_specs=pl.BlockSpec((pairs, 3 * depth), lambda s, off: (0, 0), pipeline_mode=pl.Buffered(1)),
            scratch_shapes=[pltpu.VMEM((pairs, depth), F32)],
        ),
        compiler_params=pltpu.CompilerParams(dimension_semantics=("arbitrary",), vmem_limit_bytes=48 << 20),
        cost_estimate=pl.CostEstimate(flops=12 << 30, bytes_accessed=12 << 20, transcendentals=0),
        name="experts_down",
    )(offsets, unit, w_down)


def cache_kernel(block, depth, steps, len_ref, new_ref, cache_ref, out_ref, buf, in_sem, out_sem):
    chunks = cache_ref.shape[0] // block
    slots = 2 * depth

    def read(c):
        return pltpu.make_async_copy(cache_ref.at[pl.ds(c * block, block)], buf.at[c % slots], in_sem.at[c % slots])

    def write(c):
        return pltpu.make_async_copy(buf.at[c % slots], out_ref.at[pl.ds(c * block, block)], out_sem.at[c % slots])

    for c in range(depth):
        read(c).start()

    def body(c, carry):
        @pl.when(c >= depth)
        def _():
            write(c - depth).wait()

        @pl.when(c + depth < chunks)
        def _():
            read(c + depth).start()

        read(c).wait()
        for j in range(block):
            b = c * block + j
            buf[c % slots, j, pl.ds(len_ref[b], steps)] = new_ref[b]
        write(c).start()
        return carry

    lax.fori_loop(0, chunks, body, 0)
    for k in range(depth):
        write(chunks - depth + k).wait()


def write_cache(lengths, new_rows, cache, name):
    block, depth = 8, 4
    return pl.pallas_call(
        functools.partial(cache_kernel, block, depth, new_rows.shape[1]),
        out_shape=jax.ShapeDtypeStruct(cache.shape, cache.dtype),
        in_specs=[pl.BlockSpec(memory_space=pltpu.SMEM), pl.BlockSpec(memory_space=pltpu.VMEM), pl.BlockSpec(memory_space=pltpu.HBM)],
        out_specs=pl.BlockSpec(memory_space=pltpu.HBM),
        scratch_shapes=[
            pltpu.VMEM((2 * depth, block) + cache.shape[1:], cache.dtype),
            pltpu.SemaphoreType.DMA((2 * depth,)),
            pltpu.SemaphoreType.DMA((2 * depth,)),
        ],
        compiler_params=pltpu.CompilerParams(vmem_limit_bytes=20 << 20),
        cost_estimate=pl.CostEstimate(flops=0, bytes_accessed=2 * cache.size * 2, transcendentals=0),
        name=name,
    )(lengths, new_rows, cache)


def greet(axis, peers):
    barrier = pltpu.get_barrier_semaphore()
    for peer in peers:
        pl.semaphore_signal(barrier, inc=1, device_id={axis: peer}, device_id_type=MESH)
    pl.semaphore_wait(barrier, len(peers))


def gather_kernel(axis, n, in_ref, out_ref, send_sem, recv_sem):
    me = lax.axis_index(axis)
    peers = [lax.rem(me + d, n) for d in range(1, n)]
    greet(axis, peers)
    copies = []
    for d, peer in enumerate(peers):
        copies.append(pltpu.make_async_remote_copy(src_ref=in_ref, dst_ref=out_ref.at[me], send_sem=send_sem.at[d], recv_sem=recv_sem.at[d], device_id={axis: peer}, device_id_type=MESH))
        copies[-1].start()
    out_ref[me] = in_ref[...]
    for copy in copies:
        copy.wait()


def small_gather(arr, axis, n, ident):
    return pl.pallas_call(
        functools.partial(gather_kernel, axis, n),
        out_shape=jax.ShapeDtypeStruct((n,) + arr.shape, arr.dtype),
        in_specs=[pl.BlockSpec(memory_space=pltpu.VMEM)],
        out_specs=pl.BlockSpec(memory_space=pltpu.VMEM),
        scratch_shapes=[pltpu.SemaphoreType.DMA((n - 1,)), pltpu.SemaphoreType.DMA((n - 1,))],
        compiler_params=pltpu.CompilerParams(collective_id=ident, has_side_effects=True),
        name=f"gather_{ident}",
    )(arr)


def pair_gather_kernel(axis, n, in_ref, out_ref, send_sem, recv_sem, fwd_send, fwd_recv):
    me = lax.axis_index(axis)
    partner = me + 1 - 2 * lax.rem(me, 2)
    chips = n // 2
    peers = [lax.rem(me + 2 * d, n) for d in range(1, chips)]
    greet(axis, peers + [partner])

    def copy(src, dst, send, recv, peer):
        out = pltpu.make_async_remote_copy(src_ref=src, dst_ref=dst, send_sem=send, recv_sem=recv, device_id={axis: peer}, device_id_type=MESH)
        out.start()
        return out

    first = [copy(in_ref, out_ref.at[me], send_sem.at[d], recv_sem.at[d], peer) for d, peer in enumerate(peers + [partner])]
    out_ref[me] = in_ref[...]
    second = []
    for d in range(1, chips):
        first[d - 1].wait_recv()
        origin = lax.rem(me + n - 2 * d, n)
        second.append(copy(out_ref.at[origin], out_ref.at[origin], fwd_send.at[d - 1], fwd_recv.at[d - 1], partner))
    first[-1].wait_recv()
    for item in second:
        item.wait_recv()
    for item in first + second:
        item.wait_send()


def pair_gather(arr, axis, n, ident):
    chips = n // 2
    return pl.pallas_call(
        functools.partial(pair_gather_kernel, axis, n),
        out_shape=jax.ShapeDtypeStruct((n,) + arr.shape, arr.dtype),
        in_specs=[pl.BlockSpec(memory_space=pltpu.VMEM)],
        out_specs=pl.BlockSpec(memory_space=pltpu.VMEM),
        scratch_shapes=[pltpu.SemaphoreType.DMA((chips,)), pltpu.SemaphoreType.DMA((chips,)), pltpu.SemaphoreType.DMA((chips - 1,)), pltpu.SemaphoreType.DMA((chips - 1,))],
        compiler_params=pltpu.CompilerParams(collective_id=ident, has_side_effects=True),
        name=f"pair_gather_{ident}",
    )(arr)


def sum_kernel(axis, n, in_ref, out_ref, part_ref, total_ref, send_a, recv_a, send_b, recv_b):
    me = lax.axis_index(axis)
    peers = [lax.rem(me + d, n) for d in range(1, n)]
    greet(axis, peers)
    first = []
    for d, peer in enumerate(peers):
        first.append(pltpu.make_async_remote_copy(src_ref=in_ref.at[peer], dst_ref=part_ref.at[d], send_sem=send_a.at[d], recv_sem=recv_a.at[d], device_id={axis: peer}, device_id_type=MESH))
        first[-1].start()
    for copy in first:
        copy.wait_recv()
    total = in_ref[me].astype(F32)
    for d in range(n - 1):
        total = total + part_ref[d].astype(F32)
    total_ref[...] = total.astype(total_ref.dtype)
    out_ref[me] = total_ref[...]
    second = []
    for d, peer in enumerate(peers):
        second.append(pltpu.make_async_remote_copy(src_ref=total_ref, dst_ref=out_ref.at[me], send_sem=send_b.at[d], recv_sem=recv_b.at[d], device_id={axis: peer}, device_id_type=MESH))
        second[-1].start()
    for copy in second:
        copy.wait_recv()
    for copy in first + second:
        copy.wait_send()


def small_sum(arr, axis, n, ident):
    block = (arr.shape[0] // n, arr.shape[1])
    sems = [pltpu.SemaphoreType.DMA((n - 1,))] * 4
    return pl.pallas_call(
        functools.partial(sum_kernel, axis, n),
        out_shape=jax.ShapeDtypeStruct((n,) + block, arr.dtype),
        in_specs=[pl.BlockSpec(memory_space=pltpu.VMEM)],
        out_specs=pl.BlockSpec(memory_space=pltpu.VMEM),
        scratch_shapes=[pltpu.VMEM((n - 1,) + block, arr.dtype), pltpu.VMEM(block, arr.dtype)] + sems,
        compiler_params=pltpu.CompilerParams(collective_id=ident, has_side_effects=True),
        name=f"sum_{ident}",
    )(arr.reshape((n,) + block)).reshape(arr.shape)


def scatter_kernel(axis, n, in_ref, k_ref, v_ref, out_ref, my_k_ref, my_v_ref, part_ref, acc_ref, far_ref, side_ref, near_ref, hold_ref, local_sem, store_sem, send_a, recv_a, send_b, recv_b):
    me = lax.axis_index(axis)
    core = lax.rem(me, 2)
    partner = me + 1 - 2 * core
    chips = n // 2
    turn = 4 * core - 2
    after = lax.rem(me + turn + n, n)
    ahead = lax.rem(me - turn + n, n)
    across = lax.rem(me + 2 * (chips // 2), n)
    greet(axis, [partner, after, ahead])

    def copy(src, dst, send, recv, peer):
        out = pltpu.make_async_remote_copy(src_ref=src, dst_ref=dst, send_sem=send, recv_sem=recv, device_id={axis: peer}, device_id_type=MESH)
        out.start()
        return out

    order = [across, ahead, after, me]
    first = []
    for d, place in enumerate([across, after, ahead, me]):
        first.append(copy(in_ref.at[place + partner - me], part_ref.at[d], send_a.at[d], recv_a.at[d], partner))
    part = my_k_ref.shape[0]
    reads = []
    for d, src in enumerate((k_ref, v_ref)):
        reads.append(pltpu.make_async_copy(src.at[pl.ds(me * part, part)], hold_ref.at[d], local_sem.at[d]))
        reads[-1].start()

    def pair_sum(d):
        first[d].wait_recv()
        return in_ref[order[d]].astype(F32) + part_ref[d].astype(F32)

    acc_ref[0] = pair_sum(0).astype(acc_ref.dtype)
    far = copy(acc_ref.at[0], far_ref, send_b.at[0], recv_b.at[0], after)
    acc_ref[1] = pair_sum(1).astype(acc_ref.dtype)
    side = copy(acc_ref.at[1], side_ref, send_b.at[1], recv_b.at[1], ahead)
    mid = pair_sum(2)
    far.wait_recv()
    acc_ref[2] = (mid + far_ref[...].astype(F32)).astype(acc_ref.dtype)
    near = copy(acc_ref.at[2], near_ref, send_b.at[2], recv_b.at[2], after)
    stores = []
    for d, dst in enumerate((my_k_ref, my_v_ref)):
        reads[d].wait()
        stores.append(pltpu.make_async_copy(hold_ref.at[d], dst, store_sem.at[d]))
        stores[-1].start()
    own = pair_sum(3)
    side.wait_recv()
    own = own + side_ref[...].astype(F32)
    near.wait_recv()
    out_ref[...] = (own + near_ref[...].astype(F32)).astype(out_ref.dtype)
    for item in first + [far, side, near]:
        item.wait_send()
    for item in stores:
        item.wait()


def scatter_rows(arr, k_cache, v_cache, axis, n, ident):
    rows, cols = arr.shape
    block = (rows // n, cols)
    mine = (k_cache.shape[0] // n,) + k_cache.shape[1:]
    vmem = pl.BlockSpec(memory_space=pltpu.VMEM)
    return pl.pallas_call(
        functools.partial(scatter_kernel, axis, n),
        out_shape=(jax.ShapeDtypeStruct(block, arr.dtype), jax.ShapeDtypeStruct(mine, k_cache.dtype), jax.ShapeDtypeStruct(mine, v_cache.dtype)),
        in_specs=[vmem, pl.BlockSpec(memory_space=pl.ANY), pl.BlockSpec(memory_space=pl.ANY)],
        out_specs=(vmem, pl.BlockSpec(memory_space=pltpu.HBM), pl.BlockSpec(memory_space=pltpu.HBM)),
        scratch_shapes=[pltpu.VMEM((4,) + block, arr.dtype), pltpu.VMEM((3,) + block, arr.dtype)] + [pltpu.VMEM(block, arr.dtype)] * 3
        + [pltpu.VMEM((2,) + mine, k_cache.dtype), pltpu.SemaphoreType.DMA((2,)), pltpu.SemaphoreType.DMA((2,)), pltpu.SemaphoreType.DMA((4,)), pltpu.SemaphoreType.DMA((4,)), pltpu.SemaphoreType.DMA((3,)), pltpu.SemaphoreType.DMA((3,))],
        compiler_params=pltpu.CompilerParams(collective_id=ident, has_side_effects=True, vmem_limit_bytes=40 << 20),
        name=f"scatter_{ident}",
    )(arr.reshape((n,) + block), k_cache, v_cache)


def solution(mesh):
    nx, ny = mesh.shape['x'], mesh.shape['y']
    cache_spec = P('dp', None, 'y', None)
    in_specs = (P(None, 'dp'), P('dp'), P(None, 'dp', None), P(None, 'x'), cache_spec, cache_spec, P('x'), P('x', 'y'), P('x', 'y'), P('x', 'y'), P('y', 'x'), P('x'), P('x', None), P(None, 'x', 'y'), P(None, 'x', 'y'), P(None, 'y', 'x'))
    out_specs = (P(None, 'dp', 'x'), cache_spec, cache_spec)

    def per_device(tokens, lengths, choices, emb_table, k_cache, v_cache, g_attn, w_q, w_k, w_v, w_o, g_ffn, w_router, w_act, w_lin, w_down):
        steps, batch = tokens.shape
        top = choices.shape[2]
        heads, head_dim = k_cache.shape[2], k_cache.shape[3]
        cols = heads * head_dim
        width_full = emb_table.shape[1] * nx
        experts = w_act.shape[0]
        my_x = lax.axis_index('x')
        part = batch // nx
        rows = steps * batch
        pairs = rows * top

        def to_rows(arr):
            return arr.reshape((steps, nx, part) + arr.shape[2:]).swapaxes(0, 1).reshape((rows,) + arr.shape[2:])

        def from_rows(arr):
            return arr.reshape((nx, steps, part) + arr.shape[1:]).swapaxes(0, 1).reshape((steps, batch) + arr.shape[1:])

        choice_rows = to_rows(choices)
        member = jnp.any(choice_rows[:, :, None] == jnp.arange(experts)[None, None, :], axis=1)
        member_f = member.astype(F32)
        before = (jnp.arange(rows)[None, :] < jnp.arange(rows)[:, None]).astype(BF16)
        rank = jnp.dot(before, member.astype(BF16), preferred_element_type=F32)
        counts = jnp.sum(member_f, axis=0)
        ends = jnp.cumsum(counts)
        starts = ends - counts
        place = (rank + starts[None, :]).astype(jnp.int32)
        offsets = jnp.concatenate([starts, ends[-1:]]).astype(jnp.int32)
        high = jnp.where(member, place // 128, 255).astype(BF16)
        low = jnp.where(member, place % 128, 0).astype(BF16)
        places = jnp.arange(pairs).astype(F32)
        pair_expert = (places[:, None] >= starts[None, :]) & (places[:, None] < ends[None, :])
        left = jnp.concatenate([jnp.where(pair_expert, 128.0, 0.0), jnp.where(pair_expert, 1.0, 0.0)], axis=1).astype(BF16)
        right = jnp.concatenate([high, low], axis=1)
        pick = (lax.dot_general(left, right, (((1,), (1,)), ((), ())), preferred_element_type=F32) == places[:, None]).astype(BF16)
        put = (lax.dot_general(right, left, (((1,), (1,)), ((), ())), preferred_element_type=F32) == places[None, :]).astype(BF16)
        put = lax.optimization_barrier(put)
        chunk = pairs // CHUNKS
        share = chunk // nx

        x_in = jnp.take(emb_table, to_rows(tokens), axis=0)
        normed = shard_norm(x_in, g_attn, width_full, nx, 0)
        w_qkv = jnp.concatenate([w_q, w_k, w_v], axis=1)
        proj_part = jnp.dot(normed, w_qkv, preferred_element_type=F32).astype(BF16)
        proj, my_keys, my_vals = scatter_rows(proj_part, k_cache, v_cache, 'x', nx, 6)
        my_lengths = lax.dynamic_slice_in_dim(lengths, my_x * part, part)
        my_positions = my_lengths[None, :] + jnp.arange(steps)[:, None]
        flat_positions = my_positions.reshape(-1)
        queries = rotate(proj[:, :cols].reshape(-1, heads, head_dim), flat_positions)
        new_keys = rotate(proj[:, cols:2 * cols].reshape(-1, heads, head_dim), flat_positions)
        new_vals = proj[:, 2 * cols:].reshape(-1, heads, head_dim)

        def split(arr):
            return arr.reshape(steps, part, heads, head_dim)

        mixed = attention(split(queries), split(new_keys), split(new_vals), my_keys, my_vals, my_lengths).reshape(-1, cols)
        mixed_all = pair_gather(mixed, 'x', nx, 2).reshape(rows, cols)

        new_kv = jnp.concatenate([new_keys.reshape(-1, cols), proj[:, 2 * cols:]], axis=1)
        kv_all = lax.all_gather(new_kv, 'x', axis=0, tiled=True)
        kv_all = kv_all.reshape(nx, steps, part, 2, heads, head_dim).transpose(3, 0, 2, 1, 4, 5).reshape(2, batch, steps, heads, head_dim)
        attn_part = jnp.dot(mixed_all, w_o, preferred_element_type=F32).astype(BF16)
        attn_sum = small_sum(attn_part, 'y', ny, 3)
        x_mid = (x_in.astype(F32) + attn_sum.astype(F32)).astype(BF16)
        normed2 = shard_norm(x_mid, g_ffn, width_full, nx, 1)
        normed2, new_k, new_v = lax.optimization_barrier((normed2, kv_all[0], kv_all[1]))
        k_out = write_cache(lengths, new_k, k_cache, "write_keys")
        v_out = write_cache(lengths, new_v, v_cache, "write_vals")
        logits = small_sum(jnp.dot(normed2, w_router, preferred_element_type=F32), 'x', nx, 4)
        masked = jnp.where(member, logits, -jnp.inf)
        expd = jnp.exp(masked - jnp.max(masked, axis=1, keepdims=True))
        coef = expd / jnp.sum(expd, axis=1, keepdims=True)
        width = w_act.shape[2]

        def bounds(c):
            return jnp.clip(offsets - c * chunk, 0, chunk)

        hidden = []
        for c in range(CHUNKS):
            pair_rows = jnp.dot(pick[c * chunk:(c + 1) * chunk], normed2, preferred_element_type=F32).astype(BF16)
            hidden_part = experts_up(bounds(c), pair_rows, w_act, w_lin)
            hidden.append(lax.psum_scatter(hidden_part, 'x', scatter_dimension=0, tiled=True))
        unit_all = []
        for c in range(CHUNKS):
            own_expert = lax.dynamic_slice_in_dim(pair_expert, c * chunk + my_x * share, share).astype(F32)
            own_token = lax.dynamic_slice_in_dim(pick, c * chunk + my_x * share, share).astype(F32)
            own_gate = jnp.sum(own_expert * jnp.dot(own_token, coef, precision=lax.Precision.HIGHEST, preferred_element_type=F32), axis=1, keepdims=True)
            if c == CHUNKS - 1:
                own_gate, k_out = lax.optimization_barrier((own_gate, k_out))
            act, lin = hidden[c][:, :width].astype(F32), hidden[c][:, width:].astype(F32)
            unit_all.append(lax.all_gather((own_gate * jax.nn.silu(act) * lin).astype(BF16), 'x', axis=0, tiled=True))
        terms = 0.0
        for c in range(CHUNKS):
            if c == CHUNKS - 1:
                unit_all[c], v_out = lax.optimization_barrier((unit_all[c], v_out))
            terms = terms + jnp.dot(put[:, c * chunk:(c + 1) * chunk], experts_down(bounds(c), unit_all[c], w_down), preferred_element_type=F32)
        depth = w_down.shape[2]
        moe_part = (terms[:, :depth] + terms[:, depth:2 * depth] + terms[:, 2 * depth:]).astype(BF16)
        moe_sum = small_sum(moe_part, 'y', ny, 5)
        hidden_out = (x_mid.astype(F32) + moe_sum.astype(F32)).astype(BF16)
        return from_rows(hidden_out), k_out, v_out

    return jax.shard_map(per_device, mesh=mesh, in_specs=in_specs, out_specs=out_specs, check_vma=False)
```
